32 devices in a mesh: model: 8 (over z, y), data: 4 (over x, core).
Axes of the slice: x: 2, y: 2, z: 4, core: 2. Of those that a mesh axis runs over, the one named last changes fastest.
Arguments:
- x_tokens: bfloat16 [32, 49, 768], P('data')
- y_target: bfloat16 [32, 49, 768], P('data')
- w_in: float32 [12, 768, 3072], P(None, None, 'model')
- w_out: float32 [12, 3072, 768], P(None, 'model')
Outputs:
- output 1: float32 [12, 768, 3072], P(None, None, 'model')
- output 2: float32 [12, 3072, 768], P(None, 'model')
- output 3: float32 [], replicated
All inputs are finite; a program needn't handle non-finite values.
Results may differ from the reference program's by a relative error of at most 0.00413934.
Values are sent between devices in bfloat16 or wider.
A program may use at most 1 GiB of HBM per device.

```python
import math
import jax
import jax.numpy as jnp
from jax import lax

DATA = 4
IMAGES = 8
SEQ = 49
D = 768
FF = 3072
LAYERS = 12

TOKENS = IMAGES * SEQ
BATCH = DATA * IMAGES
RHO = 0.5 * math.sqrt(D / FF)
ETA = 1.0


def setup_inputs(seed: int = 0) -> dict:
    rand_key = jax.random.key(seed)
    key_list = jax.random.split(rand_key, 7)
    x_tokens = jax.random.normal(key_list[0], (BATCH, SEQ, D), jnp.float32)
    img_mean = 1.5 * jax.random.normal(key_list[1], (BATCH, 1, D), jnp.float32)
    y_target = img_mean + 0.5 * jax.random.normal(key_list[2], (BATCH, SEQ, D), jnp.float32)
    in_scale = jax.random.uniform(key_list[3], (LAYERS, 1, 1), jnp.float32, 0.5, 2.0)
    out_scale = jax.random.uniform(key_list[4], (LAYERS, 1, 1), jnp.float32, 0.5, 1.5)
    w_in = in_scale * jax.random.normal(key_list[5], (LAYERS, D, FF), jnp.float32) / math.sqrt(D)
    w_out = out_scale * jax.random.normal(key_list[6], (LAYERS, FF, D), jnp.float32) * math.sqrt(4.0 / (FF * (LAYERS + 3)))
    return {"x_tokens": x_tokens.astype(jnp.bfloat16), "y_target": y_target.astype(jnp.bfloat16), "w_in": w_in, "w_out": w_out}


def gelu_fn(values):
    return jax.nn.gelu(values, approximate=True)


def shard_pass(w_in_b, w_out_b, x_shard, y_shard):
    def fwd_layer(hidden, layer_w):
        win_l, wout_l = layer_w
        z_bf = jnp.dot(hidden, win_l, preferred_element_type=jnp.float32).astype(jnp.bfloat16)
        act_b = gelu_fn(z_bf.astype(jnp.float32)).astype(jnp.bfloat16)
        mix_out = jnp.dot(act_b, wout_l, preferred_element_type=jnp.float32)
        new_hidden = (hidden.astype(jnp.float32) + mix_out).astype(jnp.bfloat16)
        return new_hidden, (hidden, z_bf, act_b)

    h_last, saved_acts = lax.scan(fwd_layer, x_shard, (w_in_b, w_out_b))
    residual = h_last.astype(jnp.float32) - y_shard.astype(jnp.float32)
    loss_sum = 0.5 * jnp.sum(residual * residual)
    grad_last = residual / (TOKENS * D)

    def bwd_layer(grad_h, layer_in):
        win_l, wout_l, hidden, z_bf, act_b = layer_in
        grad_b = grad_h.astype(jnp.bfloat16)
        g_out = jnp.dot(act_b.T, grad_b, preferred_element_type=jnp.float32).astype(jnp.bfloat16)
        act_grad = jnp.dot(grad_b, wout_l.T, preferred_element_type=jnp.float32)
        act_pull = jax.vjp(gelu_fn, z_bf.astype(jnp.float32))[1]
        dz_bf = act_pull(act_grad)[0].astype(jnp.bfloat16)
        g_in = jnp.dot(hidden.T, dz_bf, preferred_element_type=jnp.float32).astype(jnp.bfloat16)
        grad_prev = grad_h + jnp.dot(dz_bf, win_l.T, preferred_element_type=jnp.float32)
        return grad_prev, (g_in, g_out)

    h_saved, z_saved, act_saved = saved_acts
    grad_pair = lax.scan(bwd_layer, grad_last, (w_in_b, w_out_b, h_saved, z_saved, act_saved), reverse=True)[1]
    return loss_sum, grad_pair[0], grad_pair[1]


def mean_pass(w_in_b, w_out_b, x_tokens, y_target):
    x_shards = x_tokens.reshape(DATA, TOKENS, D)
    y_shards = y_target.reshape(DATA, TOKENS, D)

    def shard_step(carry_val, shard_pair):
        loss_acc, in_acc, out_acc = carry_val
        loss_sum, g_in, g_out = shard_pass(w_in_b, w_out_b, shard_pair[0], shard_pair[1])
        return (loss_acc + loss_sum, in_acc + g_in.astype(jnp.float32), out_acc + g_out.astype(jnp.float32)), None

    init_acc = (jnp.zeros((), jnp.float32), jnp.zeros((LAYERS, D, FF), jnp.float32), jnp.zeros((LAYERS, FF, D), jnp.float32))
    totals = lax.scan(shard_step, init_acc, (x_shards, y_shards))[0]
    return totals[0] / (DATA * TOKENS * D), totals[1] / DATA, totals[2] / DATA


def reference(x_tokens, y_target, w_in, w_out):
    first_pass = mean_pass(w_in.astype(jnp.bfloat16), w_out.astype(jnp.bfloat16), x_tokens, y_target)
    g_in = first_pass[1]
    g_out = first_pass[2]
    grad_norm = jnp.sqrt(jnp.sum(g_in * g_in) + jnp.sum(g_out * g_out))
    step_scale = RHO / grad_norm
    pert_in = (w_in + step_scale * g_in).astype(jnp.bfloat16)
    pert_out = (w_out + step_scale * g_out).astype(jnp.bfloat16)
    loss_pert, gp_in, gp_out = mean_pass(pert_in, pert_out, x_tokens, y_target)
    return w_in - ETA * gp_in, w_out - ETA * gp_out, loss_pert
```

```python
import functools
import math

import jax
import jax.numpy as jnp
from jax import lax
from jax.experimental import pallas as pl
from jax.experimental.pallas import tpu as pltpu
from jax.sharding import PartitionSpec as P

MESH = pl.DeviceIdType.MESH
RHO_SCALE = 0.5
ETA = 1.0
HALF = 6
MB_IMAGES = 2
VMEM_LIMIT = 67043328
NN = (((1,), (0,)), ((), ()))
NT = (((1,), (1,)), ((), ()))
TN = (((0,), (0,)), ((), ()))
C0 = math.sqrt(2.0 / math.pi)
C1 = 0.044715


def dot(lhs, rhs, dims):
    return lax.dot_general(lhs, rhs, dims, preferred_element_type=jnp.float32)


def chip_of(pos):
    return 2 * (pos - 1) + 3 * lax.div(5 - pos, 5) - lax.div(pos, 5)


def static_chip(pos):
    return [1, 0, 2, 4, 6, 7][pos]


def locate():
    m = lax.axis_index("model")
    d = lax.axis_index("data")
    x, core = lax.div(d, 2), lax.rem(d, 2)
    z, y = lax.div(m, 2), lax.rem(m, 2)
    pos = (1 - y) * (z + 1) + y * 5 * lax.div(z, 3)
    idle = y * (1 - lax.div(z, 3)) * jnp.minimum(z, 1)
    stage = (1 - x) * pos + x * (11 - pos)
    return m, x, core, stage, idle == 0


def stage_device(stage, core):
    plane = lax.div(stage, HALF)
    pos = (1 - plane) * stage + plane * (11 - stage)
    return chip_of(pos), plane * 2 + core


def gather_kernel(win, wout, xin, yin, a_own, c_own, x_oth, y_oth, w_send, w_recv, loc_sem, xy_send, xy_recv):
    m, x, core, stage, active = locate()
    width = win.shape[2]
    mine = x * 2 + core
    partner = (1 - x) * 2 + core
    barrier = pltpu.get_barrier_semaphore()
    for step in range(1, 8):
        pl.semaphore_signal(barrier, inc=1, device_id=(lax.rem(m + step, 8), mine), device_id_type=MESH)
    pl.semaphore_signal(barrier, inc=1, device_id=(m, partner), device_id_type=MESH)
    pl.semaphore_wait(barrier, 8)

    xy = [
        pltpu.make_async_remote_copy(src, dst, xy_send.at[i], xy_recv.at[i], device_id=(m, partner), device_id_type=MESH)
        for i, (src, dst) in enumerate(((xin, x_oth), (yin, y_oth)))
    ]
    for copy in xy:
        copy.start()

    cols = pl.ds(pl.multiple_of(m * width, width), width)

    def ends(kind, layer, sl):
        if kind == 0:
            return win.at[layer], a_own.at[:, sl]
        return wout.at[layer], c_own.at[sl, :]

    for kind in (0, 1):
        @pl.when(core == kind)
        def _(kind=kind):
            for pos in range(HALF):
                dest = static_chip(pos)
                layer = (1 - x) * pos + x * (11 - pos)
                src, dst = ends(kind, layer, cols)

                @pl.when(m != dest)
                def _():
                    pltpu.make_async_remote_copy(src, dst, w_send.at[pos], w_recv.at[m], device_id=(dest, mine), device_id_type=MESH).start()

                @pl.when(m == dest)
                def _():
                    pltpu.make_async_copy(src, dst, loc_sem).start()

            for pos in range(HALF):
                dest = static_chip(pos)
                layer = (1 - x) * pos + x * (11 - pos)
                src, dst = ends(kind, layer, cols)

                @pl.when(m != dest)
                def _():
                    pltpu.make_async_remote_copy(src, dst, w_send.at[pos], w_recv.at[m], device_id=(dest, mine), device_id_type=MESH).wait_send()

                @pl.when(m == dest)
                def _():
                    pltpu.make_async_copy(src, dst, loc_sem).wait()

            @pl.when(active)
            def _():
                for peer in range(8):
                    src, dst = ends(kind, 0, pl.ds(peer * width, width))

                    @pl.when(m != peer)
                    def _():
                        pltpu.make_async_remote_copy(src, dst, w_send.at[0], w_recv.at[peer], device_id=(m, mine), device_id_type=MESH).wait_recv()

    for copy in xy:
        copy.wait()


def pass_kernel(cfg, a_in, c_in, x_ref, y_ref, ga_ref, gc_ref, ra_ref, rc_ref, loss_ref,
                a, c, hbuf, hout, zbuf, ubuf, ebuf, eout, ebb,
                w_send, w_recv, w_loc, g_send, g_recv, hs, hr, es, er):
    rows, per_shard, n_mb, res_scale = cfg
    m, x, core, stage, active = locate()
    width = x_ref.shape[1]
    hidden = a.shape[1]
    quarter = hidden // 4
    mine = x * 2 + core
    twin = x * 2 + (1 - core)
    prev_dev = stage_device(jnp.maximum(stage - 1, 0), core)
    next_dev = stage_device(jnp.minimum(stage + 1, 11), core)
    first = stage == 0
    last = stage == 11

    def block(mb):
        return pl.ds(pl.multiple_of(mb * rows, rows), rows)

    def h_copy(mb):
        return pltpu.make_async_remote_copy(hout.at[block(mb), :], hbuf.at[block(mb), :], hs.at[mb], hr.at[mb], device_id=next_dev, device_id_type=MESH)

    def e_copy(mb):
        return pltpu.make_async_remote_copy(eout.at[block(mb), :], ebuf.at[block(mb), :], es.at[mb], er.at[mb], device_id=prev_dev, device_id_type=MESH)

    def forward(mb):
        h = hbuf[block(mb), :]
        mix = None
        for q in range(4):
            sl = slice(q * quarter, (q + 1) * quarter)
            z = dot(h, a[:, sl], NN).astype(jnp.bfloat16)
            zf = z.astype(jnp.float32)
            u = (zf * (0.5 * (1.0 + jnp.tanh(C0 * (zf + C1 * (zf * zf * zf)))))).astype(jnp.bfloat16)
            zbuf[block(mb), sl] = z
            ubuf[block(mb), sl] = u
            part = dot(u, c[sl, :], NN)
            mix = part if mix is None else mix + part
        return (h.astype(jnp.float32) + mix).astype(jnp.bfloat16)

    def backward(mb, need_back):
        e = ebuf[block(mb), :]
        eb = e.astype(jnp.bfloat16)
        ebb[block(mb), :] = eb
        back = None
        for q in range(4):
            sl = slice(q * quarter, (q + 1) * quarter)
            du = dot(eb, c[sl, :], NT)
            zf = zbuf[block(mb), sl].astype(jnp.float32)
            z2 = zf * zf
            t = jnp.tanh(C0 * (zf + C1 * (z2 * zf)))
            slope = 0.5 * (1.0 + t) + (0.5 * zf) * ((1.0 - t * t) * (C0 + (3.0 * C0 * C1) * z2))
            dz = (slope * du).astype(jnp.bfloat16)
            zbuf[block(mb), sl] = dz
            if need_back:
                part = dot(dz, a[:, sl], NT)
                back = part if back is None else back + part
        if need_back:
            eout[block(mb), :] = e + back

    shard_rows = per_shard * rows

    def grad_piece(shard, q):
        span = pl.ds(shard * shard_rows, shard_rows)
        sl = slice(q * quarter, (q + 1) * quarter)
        gc = dot(ubuf[span, sl], ebb[span, :], TN).astype(jnp.bfloat16).astype(jnp.float32)
        ga = dot(hbuf[span, :], zbuf[span, sl], TN).astype(jnp.bfloat16).astype(jnp.float32)
        if shard == 0:
            gc_ref[sl, :] = gc
            ga_ref[:, sl] = ga
        else:
            gc_ref[sl, :] = gc_ref[sl, :] + gc
            ga_ref[:, sl] = ga_ref[:, sl] + ga

    a_loc = pltpu.make_async_copy(a_in, a, w_loc)
    c_loc = pltpu.make_async_copy(c_in, c, w_loc)
    a_rem = pltpu.make_async_remote_copy(a_in, a, w_send, w_recv, device_id=(m, twin), device_id_type=MESH)
    c_rem = pltpu.make_async_remote_copy(c_in, c, w_send, w_recv, device_id=(m, twin), device_id_type=MESH)
    a_grad = pltpu.make_async_remote_copy(ga_ref, ra_ref, g_send, g_recv, device_id=(m, twin), device_id_type=MESH)
    c_grad = pltpu.make_async_remote_copy(gc_ref, rc_ref, g_send, g_recv, device_id=(m, twin), device_id_type=MESH)

    barrier = pltpu.get_barrier_semaphore()
    loss_ref[...] = jnp.zeros_like(loss_ref)

    @pl.when(active)
    def _():
        pl.semaphore_signal(barrier, inc=1, device_id=(m, twin), device_id_type=MESH)

        @pl.when(stage > 0)
        def _():
            pl.semaphore_signal(barrier, inc=1, device_id=prev_dev, device_id_type=MESH)

        @pl.when(stage < 11)
        def _():
            pl.semaphore_signal(barrier, inc=1, device_id=next_dev, device_id_type=MESH)

        pl.semaphore_wait(barrier, 3 - lax.div(11 - stage, 11) - lax.div(stage, 11))

        @pl.when(core == 0)
        def _():
            a_rem.start()
            a_loc.start()

        @pl.when(core == 1)
        def _():
            c_rem.start()
            c_loc.start()

        @pl.when(first)
        def _():
            hbuf[...] = x_ref[...]

        @pl.when(core == 0)
        def _():
            a_loc.wait()
            a_rem.wait_send()
            c_rem.wait_recv()

        @pl.when(core == 1)
        def _():
            c_loc.wait()
            c_rem.wait_send()
            a_rem.wait_recv()

        def forward_step(mb, carry):
            @pl.when(stage > 0)
            def _():
                h_copy(mb).wait_recv()

            new_h = forward(mb)

            @pl.when(stage < 11)
            def _():
                hout[block(mb), :] = new_h
                h_copy(mb).start()

            @pl.when(last)
            def _():
                res = new_h.astype(jnp.float32) - y_ref[block(mb), :].astype(jnp.float32)
                loss_ref[...] = loss_ref[...] + jnp.sum(res * res, axis=0, keepdims=True)
                ebuf[block(mb), :] = res / res_scale
                backward(mb, True)
                e_copy(mb).start()

            return carry

        lax.fori_loop(0, n_mb, forward_step, 0)

        for shard in range(2):
            def backward_step(mb, carry):
                @pl.when(stage < 11)
                def _():
                    e_copy(mb).wait_recv()
                    backward(mb, True)

                    @pl.when(stage > 0)
                    def _():
                        e_copy(mb).start()

                return carry

            if shard == 0:
                lax.fori_loop(0, per_shard, backward_step, 0)
            else:
                for j in range(4):
                    lo, hi = n_mb // 2 + per_shard * j // 4, n_mb // 2 + per_shard * (j + 1) // 4
                    lax.fori_loop(lo, hi, backward_step, 0)
                    grad_piece(0, j)
        for q in range(4):
            grad_piece(1, q)

        @pl.when(core == 0)
        def _():
            c_grad.start()

        @pl.when(core == 1)
        def _():
            a_grad.start()

        def drain(mb, carry):
            @pl.when(stage < 11)
            def _():
                h_copy(mb).wait_send()

            @pl.when(stage > 0)
            def _():
                e_copy(mb).wait_send()

            return carry

        lax.fori_loop(0, n_mb, drain, 0)

        @pl.when(core == 0)
        def _():
            c_grad.wait_send()
            a_grad.wait_recv()

        @pl.when(core == 1)
        def _():
            a_grad.wait_send()
            c_grad.wait_recv()


def scatter_kernel(ga, gc, gin, gout, s1, r1, s2, r2, s3, r3, loc_sem):
    m, x, core, stage, active = locate()
    width = gin.shape[2]
    mine = x * 2 + core
    across = (1 - x) * 2 + core
    twin = x * 2 + (1 - core)
    barrier = pltpu.get_barrier_semaphore()
    for step in range(1, 8):
        pl.semaphore_signal(barrier, inc=1, device_id=(lax.rem(m + step, 8), mine), device_id_type=MESH)
    for other in (across, twin):
        pl.semaphore_signal(barrier, inc=1, device_id=(m, other), device_id_type=MESH)
    pl.semaphore_wait(barrier, 9)

    def piece(kind, peer):
        return ga.at[:, pl.ds(peer * width, width)] if kind == 0 else gc.at[pl.ds(peer * width, width), :]

    for kind in (0, 1):
        @pl.when(core == kind)
        def _(kind=kind):
            dst = gin if kind == 0 else gout
            other_dst = gout if kind == 0 else gin

            def first_hop(peer, layer, slot):
                return pltpu.make_async_remote_copy(piece(kind, peer), dst.at[layer], s1.at[peer], r1.at[slot], device_id=(peer, mine), device_id_type=MESH)

            def cross(layer, slot):
                return pltpu.make_async_remote_copy(dst.at[layer], dst.at[layer], s2.at[slot], r2.at[slot], device_id=(m, across), device_id_type=MESH)

            def to_twin(layer):
                return pltpu.make_async_remote_copy(dst.at[layer], dst.at[layer], s3.at[layer], r3.at[layer], device_id=(m, twin), device_id_type=MESH)

            def from_twin(layer):
                return pltpu.make_async_remote_copy(other_dst.at[layer], other_dst.at[layer], s3.at[layer], r3.at[layer], device_id=(m, twin), device_id_type=MESH)

            @pl.when(active)
            def _():
                for peer in range(8):
                    @pl.when(m != peer)
                    def _():
                        first_hop(peer, stage, stage - x * HALF).start()

                    @pl.when(m == peer)
                    def _():
                        pltpu.make_async_copy(piece(kind, peer), dst.at[stage], loc_sem).start()

            for slot in range(HALF):
                layer = x * HALF + slot
                is_mine = jnp.logical_and(active, stage == layer)

                @pl.when(is_mine)
                def _():
                    pltpu.make_async_copy(piece(kind, 0), dst.at[stage], loc_sem).wait()

                @pl.when(jnp.logical_not(is_mine))
                def _():
                    first_hop(0, layer, slot).wait_recv()

                cross(layer, slot).start()
                to_twin(layer).start()
            for slot in range(HALF):
                layer = (1 - x) * HALF + slot
                cross(layer, slot).wait_recv()
                to_twin(layer).start()
            for layer in range(2 * HALF):
                from_twin(layer).wait_recv()

            @pl.when(active)
            def _():
                for peer in range(8):
                    @pl.when(m != peer)
                    def _():
                        first_hop(peer, stage, stage - x * HALF).wait_send()

            for slot in range(HALF):
                cross(x * HALF + slot, slot).wait_send()
            for layer in range(2 * HALF):
                to_twin(layer).wait_send()


def comm_params(ident):
    return pltpu.CompilerParams(collective_id=ident, has_side_effects=True, vmem_limit_bytes=VMEM_LIMIT)


def any_spec(count):
    return [pl.BlockSpec(memory_space=pl.ANY)] * count


def vmem_spec(count):
    return [pl.BlockSpec(memory_space=pltpu.VMEM)] * count


def gather_blocks(win, wout, xin, yin):
    layers, depth, width = win.shape
    hidden = width * 8
    shape = jax.ShapeDtypeStruct
    dma = pltpu.SemaphoreType.DMA
    return pl.pallas_call(
        gather_kernel,
        out_shape=[shape((depth, hidden), win.dtype), shape((hidden, depth), win.dtype), shape(xin.shape, xin.dtype), shape(yin.shape, yin.dtype)],
        in_specs=any_spec(4),
        out_specs=any_spec(4),
        scratch_shapes=[dma((HALF,)), dma((8,)), dma, dma((2,)), dma((2,))],
        compiler_params=pltpu.CompilerParams(collective_id=0, has_side_effects=True),
        name="gather_blocks",
    )(win, wout, xin, yin)


def run_pass(a_in, c_in, x_mb, y_mb, rows, per_shard, res_scale, ident):
    depth, hidden = a_in.shape
    total = x_mb.shape[0]
    n_mb = total // rows
    shape = jax.ShapeDtypeStruct
    dma = pltpu.SemaphoreType.DMA
    f32, bf16 = jnp.float32, jnp.bfloat16
    return pl.pallas_call(
        functools.partial(pass_kernel, (rows, per_shard, n_mb, res_scale)),
        out_shape=[shape((depth, hidden), f32), shape((hidden, depth), f32), shape((depth, hidden), f32), shape((hidden, depth), f32), shape((1, depth), f32)],
        in_specs=any_spec(2) + vmem_spec(2),
        out_specs=vmem_spec(2) + any_spec(2) + vmem_spec(1),
        scratch_shapes=[
            pltpu.VMEM((depth, hidden), bf16),
            pltpu.VMEM((hidden, depth), bf16),
            pltpu.VMEM((total, depth), bf16),
            pltpu.VMEM((total, depth), bf16),
            pltpu.VMEM((total, hidden), bf16),
            pltpu.VMEM((total, hidden), bf16),
            pltpu.VMEM((total, depth), f32),
            pltpu.VMEM((total, depth), f32),
            pltpu.VMEM((total, depth), bf16),
            dma, dma, dma, dma, dma,
            dma((n_mb,)), dma((n_mb,)), dma((n_mb,)), dma((n_mb,)),
        ],
        compiler_params=comm_params(ident),
        name="pipeline_pass",
    )(a_in, c_in, x_mb, y_mb)


def scatter_grads(ga, gc, layers):
    depth, hidden = ga.shape
    width = hidden // 8
    shape = jax.ShapeDtypeStruct
    dma = pltpu.SemaphoreType.DMA
    return pl.pallas_call(
        scatter_kernel,
        out_shape=[shape((layers, depth, width), ga.dtype), shape((layers, width, depth), ga.dtype)],
        in_specs=any_spec(2),
        out_specs=any_spec(2),
        scratch_shapes=[dma((8,)), dma((HALF,)), dma((HALF,)), dma((HALF,)), dma((2 * HALF,)), dma((2 * HALF,)), dma],
        compiler_params=pltpu.CompilerParams(collective_id=3, has_side_effects=True),
        name="scatter_grads",
    )(ga, gc)


def solution(mesh):
    act_spec = P("data", None, None)
    in_spec = P(None, None, "model")
    out_spec = P(None, "model", None)

    def sam_step(x_tokens, y_target, w_in, w_out):
        rho = RHO_SCALE * math.sqrt(x_tokens.shape[-1] / w_in.shape[-1])
        elem_total = x_tokens.size
        n_data = mesh.shape["data"]

        def local_step(x_blk, y_blk, win_loc, wout_loc):
            layers = win_loc.shape[0]
            images, seq, depth = x_blk.shape
            m, x, core, stage, active = locate()
            raw = MB_IMAGES * seq
            rows = (raw + 15) // 16 * 16
            per_shard = images // MB_IMAGES

            def flat(blk):
                mbs = blk.reshape(per_shard, raw, depth)
                return jnp.pad(mbs, ((0, 0), (0, rows - raw), (0, 0))).reshape(per_shard * rows, depth)

            x_own, y_own = flat(x_blk), flat(y_blk)
            a_own, c_own, x_oth, y_oth = gather_blocks(win_loc, wout_loc, x_own, y_own)

            def both(own, oth):
                return jnp.where(x == 0, jnp.concatenate([own, oth]), jnp.concatenate([oth, own]))

            x_mb, y_mb = both(x_own, x_oth), both(y_own, y_oth)
            res_scale = float(images * seq * depth)

            def mean_pass(a_w, c_w, ident):
                ga, gc, ra, rc, loss = run_pass(a_w, c_w, x_mb, y_mb, rows, per_shard, res_scale, ident)
                return (ga + ra) / n_data, (gc + rc) / n_data, loss

            g_a, g_c, _ = mean_pass(a_own.astype(jnp.bfloat16), c_own.astype(jnp.bfloat16), 1)
            sq_a = jnp.where(jnp.logical_and(active, core == 0), jnp.sum(g_a * g_a), 0.0)
            sq_c = jnp.where(jnp.logical_and(active, core == 1), jnp.sum(g_c * g_c), 0.0)
            step_scale = rho / jnp.sqrt(lax.psum(sq_a + sq_c, ("model", "data")))
            pert_a = (a_own + step_scale * g_a).astype(jnp.bfloat16)
            pert_c = (c_own + step_scale * g_c).astype(jnp.bfloat16)
            g2_a, g2_c, loss = mean_pass(pert_a, pert_c, 2)
            loss_here = jnp.where(jnp.logical_and(active, stage == 11), 0.5 * jnp.sum(loss), 0.0)
            loss_val = lax.psum(loss_here, ("model", "data")) / elem_total
            grad_in, grad_out = scatter_grads(g2_a, g2_c, layers)
            return win_loc - ETA * grad_in, wout_loc - ETA * grad_out, loss_val

        stepper = jax.shard_map(local_step, mesh=mesh, in_specs=(act_spec, act_spec, in_spec, out_spec), out_specs=(in_spec, out_spec, P()), check_vma=False)
        return stepper(x_tokens, y_target, w_in, w_out)

    return sam_step
```

```python
import functools
import math

import jax
import jax.numpy as jnp
from jax import lax
from jax.experimental import pallas as pl
from jax.experimental.pallas import tpu as pltpu
from jax.sharding import PartitionSpec as P

MESH = pl.DeviceIdType.MESH
RHO_SCALE = 0.5
ETA = 1.0
HALF = 6
MB_IMAGES = 2
VMEM_LIMIT = 67043328
NN = (((1,), (0,)), ((), ()))
NT = (((1,), (1,)), ((), ()))
TN = (((0,), (0,)), ((), ()))
C0 = math.sqrt(2.0 / math.pi)
C1 = 0.044715
CHIPS = (1, 0, 2, 4, 6, 7)
STRIP = 128


def dot(lhs, rhs, dims):
    return lax.dot_general(lhs, rhs, dims, preferred_element_type=jnp.float32)


def chip_of(pos):
    return 2 * (pos - 1) + 3 * lax.div(5 - pos, 5) - lax.div(pos, 5)


def locate():
    m = lax.axis_index("model")
    d = lax.axis_index("data")
    x, core = lax.div(d, 2), lax.rem(d, 2)
    z, y = lax.div(m, 2), lax.rem(m, 2)
    pos = (1 - y) * (z + 1) + y * 5 * lax.div(z, 3)
    idle = y * (1 - lax.div(z, 3)) * jnp.minimum(z, 1)
    stage = (1 - x) * pos + x * (11 - pos)
    return m, x, core, stage, idle == 0


def stage_device(stage, core):
    plane = lax.div(stage, HALF)
    pos = (1 - plane) * stage + plane * (11 - stage)
    return chip_of(pos), plane * 2 + core


def step_kernel(cfg, win, wout, xin, yin,
                gin, gout, a_own, c_own, loss_out,
                a, c, ga, gc, rem, xbuf, ybuf, hbuf, hout, zbuf, ubuf, ebuf, eout, ebb,
                acc, nrm_send, nrm, loss_send,
                w_send, w_recv, w_loc, xy_send, xy_recv, xy_loc, stage_loc, t_send, t_recv, g_send, g_recv,
                hs, hr, es, er, stagger, n_send, n_recv, l_send, l_recv,
                s1, r1, s2, r2, s3, r3, s_loc):
    rows, per_shard, n_mb, res_scale, rho, n_data = cfg
    m, x, core, stage, active = locate()
    depth, hidden = a.shape
    width = hidden // 8
    quarter = hidden // 4
    strips = quarter // STRIP
    shard_rows = per_shard * rows
    mine = x * 2 + core
    across = (1 - x) * 2 + core
    twin = x * 2 + (1 - core)
    prev_dev = stage_device(jnp.maximum(stage - 1, 0), core)
    next_dev = stage_device(jnp.minimum(stage + 1, 11), core)
    last = stage == 11

    def remote(src, dst, send, recv, dev):
        return pltpu.make_async_remote_copy(src, dst, send, recv, device_id=dev, device_id_type=MESH)

    barrier = pltpu.get_barrier_semaphore()
    here = m * 4 + mine
    for step in range(1, 32):
        there = lax.rem(here + step, 32)
        pl.semaphore_signal(barrier, inc=1, device_id=(lax.div(there, 4), lax.rem(there, 4)), device_id_type=MESH)
    pl.semaphore_wait(barrier, 31)

    def weight_ends(kind, layer, shard):
        sl = pl.ds(pl.multiple_of(shard * width, width), width)
        return (win.at[layer], a_own.at[:, sl]) if kind == 0 else (wout.at[layer], c_own.at[sl, :])

    def weight_copy(kind, j, shard):
        layer = x * HALF + j
        src, dst = weight_ends(kind, layer, shard)
        dest = chip_of((1 - x) * j + x * (5 - j))
        return dest, remote(src, dst, w_send.at[j], w_recv.at[shard], (dest, mine)), pltpu.make_async_copy(src, dst, w_loc)

    for kind in (0, 1):
        @pl.when(core == kind)
        def _(kind=kind):
            for j in range(HALF):
                dest, far, near = weight_copy(kind, j, m)

                @pl.when(m != dest)
                def _():
                    far.start()

                @pl.when(m == dest)
                def _():
                    near.start()

    own_rows = pl.ds(pl.multiple_of(x * shard_rows, shard_rows), shard_rows)
    xy_far = [remote(src, dst.at[own_rows, :], xy_send.at[i], xy_recv.at[i], (m, across)) for i, (src, dst) in enumerate(((xin, xbuf), (yin, ybuf)))]
    xy_near = [pltpu.make_async_copy(src, dst.at[own_rows, :], xy_loc.at[i]) for i, (src, dst) in enumerate(((xin, xbuf), (yin, ybuf)))]
    for copy in xy_far + xy_near:
        copy.start()
    for copy in xy_near + xy_far:
        copy.wait()

    def piece(kind, ref_a, ref_c, q):
        sl = pl.ds(pl.multiple_of(q * quarter, quarter), quarter)
        return ref_a.at[:, sl] if kind == 0 else ref_c.at[sl, :]

    def strip(kind, ref_a, ref_c, q, i):
        cols = pl.ds(pl.multiple_of(q * quarter, quarter), quarter)
        if kind == 0:
            return ref_a, (pl.ds(pl.multiple_of(i * STRIP, STRIP), STRIP), cols)
        return ref_c, (pl.ds(pl.multiple_of(q * quarter + i * STRIP, STRIP), STRIP), slice(None))

    def strip_rows(i):
        return pl.ds(pl.multiple_of(i * STRIP, STRIP), STRIP)

    stagings = (ebuf, eout)

    def master_copy(kind, q):
        return pltpu.make_async_copy(piece(kind, a_own, c_own, q), stagings[q % 2].at[pl.ds(0, depth), :], stage_loc.at[q % 2])

    def twin_copy(kind, q):
        ref = piece(kind, a, c, q)
        return remote(ref, ref, t_send.at[q], t_recv.at[q], (m, twin))

    def grad_copy(kind, q):
        return remote(piece(kind, ga, gc, q), rem.at[q], g_send.at[q], g_recv.at[q], (m, twin))

    def load_weights(kind, scale):
        for q in range(4):
            if scale is None or q >= 2:
                master_copy(kind, q).start() if scale is not None else None
            if scale is None:
                for shard in (2 * q, 2 * q + 1):
                    far = remote(weight_ends(kind, 0, shard)[0], weight_ends(kind, 0, shard)[1], w_send.at[0], w_recv.at[shard], (m, mine))

                    @pl.when(m != shard)
                    def _():
                        far.wait_recv()

                    @pl.when(m == shard)
                    def _():
                        pltpu.make_async_copy(weight_ends(kind, 0, shard)[0], weight_ends(kind, 0, shard)[1], w_loc).wait()

                master_copy(kind, q).start()
            master_copy(kind, q).wait()

            def round_strip(i, carry):
                dst, where = strip(kind, a, c, q, i)
                value = stagings[q % 2][strip_rows(i), :]
                if scale is not None:
                    src, _ = strip(kind, ga, gc, q, i)
                    value = value + scale * src[where]
                dst[where] = value.astype(jnp.bfloat16)
                return carry

            lax.fori_loop(0, strips, round_strip, 0)
            twin_copy(kind, q).start()
        for q in range(4):
            twin_copy(kind, q).wait_send()
        for q in range(4):
            twin_copy(1 - kind, q).wait_recv()

    def block(mb):
        return pl.ds(pl.multiple_of(mb * rows, rows), rows)

    def h_copy(mb):
        return remote(hout.at[block(mb), :], hbuf.at[block(mb), :], hs.at[mb], hr.at[mb], next_dev)

    def e_copy(mb):
        return remote(eout.at[block(mb), :], ebuf.at[block(mb), :], es.at[mb], er.at[mb], prev_dev)

    def forward(mb):
        h = hbuf[block(mb), :]
        mix = None
        for q in range(4):
            sl = slice(q * quarter, (q + 1) * quarter)
            z = dot(h, a[:, sl], NN).astype(jnp.bfloat16)
            zf = z.astype(jnp.float32)
            u = (zf * (0.5 * (1.0 + jnp.tanh(C0 * (zf + C1 * (zf * zf * zf)))))).astype(jnp.bfloat16)
            zbuf[block(mb), sl] = z
            ubuf[block(mb), sl] = u
            part = dot(u, c[sl, :], NN)
            mix = part if mix is None else mix + part
        return (h.astype(jnp.float32) + mix).astype(jnp.bfloat16)

    def backward(mb):
        e = ebuf[block(mb), :]
        eb = e.astype(jnp.bfloat16)
        ebb[block(mb), :] = eb
        back = None
        for q in range(4):
            sl = slice(q * quarter, (q + 1) * quarter)
            du = dot(eb, c[sl, :], NT)
            zf = zbuf[block(mb), sl].astype(jnp.float32)
            z2 = zf * zf
            t = jnp.tanh(C0 * (zf + C1 * (z2 * zf)))
            slope = 0.5 * (1.0 + t) + (0.5 * zf) * ((1.0 - t * t) * (C0 + (3.0 * C0 * C1) * z2))
            dz = (slope * du).astype(jnp.bfloat16)
            zbuf[block(mb), sl] = dz
            part = dot(dz, a[:, sl], NT)
            back = part if back is None else back + part
        eout[block(mb), :] = e + back

    def grad_piece(shard, q):
        span = pl.ds(shard * shard_rows, shard_rows)
        sl = pl.ds(pl.multiple_of(q * quarter, quarter), quarter)
        d_out = dot(ubuf[span, sl], ebb[span, :], TN).astype(jnp.bfloat16).astype(jnp.float32)
        gc[sl, :] = d_out if shard == 0 else gc[sl, :] + d_out
        d_in = dot(hbuf[span, :], zbuf[span, sl], TN).astype(jnp.bfloat16).astype(jnp.float32)
        ga[:, sl] = d_in if shard == 0 else ga[:, sl] + d_in

    def on_core(fn):
        for kind in (0, 1):
            @pl.when(core == kind)
            def _(kind=kind):
                fn(kind)

    def run_pass(p, carry):
        acc[...] = jnp.zeros_like(acc)

        @pl.when(stage == 0)
        def _():
            hbuf[...] = xbuf[...]

            @pl.when(core == 1)
            def _():
                pl.semaphore_wait(stagger, 1)

        def forward_step(mb, carry):
            @pl.when(stage > 0)
            def _():
                h_copy(mb).wait_recv()

            new_h = forward(mb)

            @pl.when(stage < 11)
            def _():
                hout[block(mb), :] = new_h
                h_copy(mb).start()

            @pl.when(jnp.logical_and(stage == 0, jnp.logical_and(core == 0, mb == 0)))
            def _():
                pl.semaphore_signal(stagger, inc=1, device_id=(m, twin), device_id_type=MESH)

            @pl.when(last)
            def _():
                res = new_h.astype(jnp.float32) - ybuf[block(mb), :].astype(jnp.float32)
                acc[...] = acc[...] + jnp.sum(res * res, axis=0, keepdims=True)
                ebuf[block(mb), :] = res / res_scale
                backward(mb)
                e_copy(mb).start()

            return carry

        lax.fori_loop(0, n_mb, forward_step, 0)

        def fold(dst):
            total = acc[:, 0:128]
            for i in range(1, depth // 128):
                total = total + acc[:, i * 128:(i + 1) * 128]
            dst[...] = jnp.broadcast_to(total, dst.shape)

        @pl.when(jnp.logical_and(last, p == 1))
        def _():
            fold(loss_send)
            for step in range(32):
                pltpu_copy = remote(loss_send, loss_out.at[core], l_send.at[step], l_recv.at[core], (step // 4, step % 4))

                @pl.when(here != step)
                def _():
                    pltpu_copy.start()

            loss_out[core] = loss_send[...]
            for step in range(32):
                pltpu_copy = remote(loss_send, loss_out.at[core], l_send.at[step], l_recv.at[core], (step // 4, step % 4))

                @pl.when(here != step)
                def _():
                    pltpu_copy.wait_send()

        def backward_step(mb):
            @pl.when(stage < 11)
            def _():
                e_copy(mb).wait_recv()
                backward(mb)

                @pl.when(stage > 0)
                def _():
                    e_copy(mb).start()

        def first_shard(mb, carry):
            backward_step(mb)
            return carry

        def second_shard(mb, carry):
            backward_step(per_shard + mb)
            grad_piece(0, mb)
            return carry

        def tail_grads(q, carry):
            grad_piece(1, q)
            on_core(lambda kind: grad_copy(1 - kind, q).start())
            return carry

        lax.fori_loop(0, per_shard, first_shard, 0)
        lax.fori_loop(0, per_shard, second_shard, 0)
        lax.fori_loop(0, 4, tail_grads, 0)

        def drain(mb, carry):
            @pl.when(stage < 11)
            def _():
                h_copy(mb).wait_send()

            @pl.when(stage > 0)
            def _():
                e_copy(mb).wait_send()

            return carry

        lax.fori_loop(0, n_mb, drain, 0)

        def between(kind):
            for q in range(2):
                master_copy(kind, q).start()
            acc[...] = jnp.zeros_like(acc)

            def total_quarter(q, carry):
                grad_copy(kind, q).wait_recv()

                def total_strip(i, carry):
                    ref, where = strip(kind, ga, gc, q, i)
                    total = (ref[where] + rem[q, strip_rows(i), :]) / n_data
                    ref[where] = total
                    acc[...] = acc[...] + jnp.sum(total * total, axis=0, keepdims=True)
                    return carry

                return lax.fori_loop(0, strips, total_strip, carry)

            lax.fori_loop(0, 4, total_quarter, 0)
            fold(nrm_send)
            slot = stage * 2 + core

            def norm_copies():
                for s in range(12):
                    chip = CHIPS[s] if s < HALF else CHIPS[11 - s]
                    for k in range(2):
                        dev = (chip, (s // HALF) * 2 + k)
                        yield s * 2 + k, remote(nrm_send, nrm.at[slot], n_send.at[s * 2 + k], n_recv.at[slot], dev)

            for i, copy in norm_copies():
                @pl.when(slot != i)
                def _():
                    copy.start()

            nrm[slot] = nrm_send[...]
            for i, copy in norm_copies():
                @pl.when(slot != i)
                def _():
                    copy.wait_send()
                    remote(nrm_send, nrm.at[i], n_send.at[i], n_recv.at[i], (m, mine)).wait_recv()

            square = jnp.sum(jnp.sum(nrm[:, 0, :], axis=0, keepdims=True), axis=1, keepdims=True)
            for q in range(4):
                grad_copy(1 - kind, q).wait_send()
            load_weights(kind, rho / jnp.sqrt(square))

        @pl.when(p == 0)
        def _():
            on_core(between)

        return carry

    @pl.when(active)
    def _():
        on_core(lambda kind: load_weights(kind, None))
        lax.fori_loop(0, 2, run_pass, 0)

    def scatter(kind):
        dst = gin if kind == 0 else gout
        other_dst = gout if kind == 0 else gin

        def ends(peer):
            sl = pl.ds(pl.multiple_of(peer * width, width), width)
            return ga.at[:, sl] if kind == 0 else gc.at[sl, :]

        def first_hop(peer, layer, slot):
            return remote(ends(peer), dst.at[layer], s1.at[peer], r1.at[slot], (peer, mine))

        def cross(layer, slot):
            return remote(dst.at[layer], dst.at[layer], s2.at[slot], r2.at[slot], (m, across))

        def to_twin(layer):
            return remote(dst.at[layer], dst.at[layer], s3.at[layer], r3.at[layer], (m, twin))

        def from_twin(layer):
            return remote(other_dst.at[layer], other_dst.at[layer], s3.at[layer], r3.at[layer], (m, twin))

        @pl.when(active)
        def _():
            def send_quarter(q, carry):
                grad_copy(kind, q).wait_recv()

                def total_strip(i, carry):
                    ref, where = strip(kind, ga, gc, q, i)
                    ref[where] = (ref[where] + rem[q, strip_rows(i), :]) / n_data
                    return carry

                lax.fori_loop(0, strips, total_strip, 0)
                for k in range(2):
                    peer = 2 * q + k

                    @pl.when(m != peer)
                    def _():
                        first_hop(peer, stage, stage - x * HALF).start()

                    @pl.when(m == peer)
                    def _():
                        pltpu.make_async_copy(ends(peer), dst.at[stage], s_loc).start()

                return carry

            lax.fori_loop(0, 4, send_quarter, 0)

        for slot in reversed(range(HALF)):
            layer = x * HALF + slot
            is_mine = jnp.logical_and(active, stage == layer)

            @pl.when(is_mine)
            def _():
                pltpu.make_async_copy(ends(0), dst.at[layer], s_loc).wait()

            @pl.when(jnp.logical_not(is_mine))
            def _():
                first_hop(0, layer, slot).wait_recv()

            cross(layer, slot).start()
            to_twin(layer).start()
        for slot in reversed(range(HALF)):
            layer = (1 - x) * HALF + slot
            cross(layer, slot).wait_recv()
            to_twin(layer).start()
        for layer in range(2 * HALF):
            from_twin(layer).wait_recv()

        @pl.when(active)
        def _():
            for peer in range(8):
                @pl.when(m != peer)
                def _():
                    first_hop(peer, stage, stage - x * HALF).wait_send()

            for q in range(4):
                grad_copy(1 - kind, q).wait_send()

        for slot in range(HALF):
            cross(x * HALF + slot, slot).wait_send()
        for layer in range(2 * HALF):
            to_twin(layer).wait_send()

        for j in range(HALF):
            dest, far, _ = weight_copy(kind, j, m)

            @pl.when(m != dest)
            def _():
                far.wait_send()

    on_core(scatter)

    for k in range(2):
        @pl.when(jnp.logical_not(jnp.logical_and(active, jnp.logical_and(last, core == k))))
        def _():
            remote(loss_send, loss_out.at[k], l_send.at[0], l_recv.at[k], (m, mine)).wait_recv()


def run_step(win, wout, xin, yin, rows, per_shard, res_scale, rho, n_data):
    layers, depth, width = win.shape
    hidden = width * 8
    total = 2 * per_shard * rows
    n_mb = 2 * per_shard
    shape = jax.ShapeDtypeStruct
    dma = pltpu.SemaphoreType.DMA
    f32, bf16 = jnp.float32, jnp.bfloat16
    any_space = pl.BlockSpec(memory_space=pl.ANY)
    return pl.pallas_call(
        functools.partial(step_kernel, (rows, per_shard, n_mb, res_scale, rho, n_data)),
        out_shape=[shape(win.shape, f32), shape(wout.shape, f32), shape((depth, hidden), f32), shape((hidden, depth), f32), shape((2, 8, 128), f32)],
        in_specs=[any_space] * 4,
        out_specs=[any_space] * 4 + [pl.BlockSpec(memory_space=pltpu.VMEM)],
        scratch_shapes=[
            pltpu.VMEM((depth, hidden), bf16),
            pltpu.VMEM((hidden, depth), bf16),
            pltpu.VMEM((depth, hidden), f32),
            pltpu.VMEM((hidden, depth), f32),
            pltpu.VMEM((4, depth, hidden // 4), f32) if depth == hidden // 4 else pltpu.VMEM((4, depth, depth), f32),
            pltpu.VMEM((total, depth), bf16),
            pltpu.VMEM((total, depth), bf16),
            pltpu.VMEM((total, depth), bf16),
            pltpu.VMEM((total, depth), bf16),
            pltpu.VMEM((total, hidden), bf16),
            pltpu.VMEM((total, hidden), bf16),
            pltpu.VMEM((total, depth), f32),
            pltpu.VMEM((total, depth), f32),
            pltpu.VMEM((total, depth), bf16),
            pltpu.VMEM((1, depth), f32),
            pltpu.VMEM((8, 128), f32),
            pltpu.VMEM((24, 8, 128), f32),
            pltpu.VMEM((8, 128), f32),
            dma((HALF,)), dma((8,)), dma, dma((2,)), dma((2,)), dma((2,)), dma((2,)), dma((4,)), dma((4,)), dma((4,)), dma((4,)),
            dma((n_mb,)), dma((n_mb,)), dma((n_mb,)), dma((n_mb,)), pltpu.SemaphoreType.REGULAR,
            dma((24,)), dma((24,)), dma((32,)), dma((2,)),
            dma((8,)), dma((HALF,)), dma((HALF,)), dma((HALF,)), dma((2 * HALF,)), dma((2 * HALF,)), dma,
        ],
        compiler_params=pltpu.CompilerParams(collective_id=0, has_side_effects=True, vmem_limit_bytes=VMEM_LIMIT),
        name="sam_step",
    )(win, wout, xin, yin)


def solution(mesh):
    act_spec = P("data", None, None)
    in_spec = P(None, None, "model")
    out_spec = P(None, "model", None)

    def sam_step(x_tokens, y_target, w_in, w_out):
        rho = RHO_SCALE * math.sqrt(x_tokens.shape[-1] / w_in.shape[-1])
        elem_total = x_tokens.size
        n_data = mesh.shape["data"]

        def local_step(x_blk, y_blk, win_loc, wout_loc):
            images, seq, depth = x_blk.shape
            raw = MB_IMAGES * seq
            rows = (raw + 15) // 16 * 16
            per_shard = images // MB_IMAGES

            def flat(blk):
                mbs = blk.reshape(per_shard, raw, depth)
                return jnp.pad(mbs, ((0, 0), (0, rows - raw), (0, 0))).reshape(per_shard * rows, depth)

            res_scale = float(images * seq * depth)
            grad_in, grad_out, _, _, loss = run_step(win_loc, wout_loc, flat(x_blk), flat(y_blk), rows, per_shard, res_scale, rho, n_data)
            loss_val = 0.5 * jnp.sum(loss[:, 0, :]) / elem_total
            return win_loc - ETA * grad_in, wout_loc - ETA * grad_out, loss_val

        stepper = jax.shard_map(local_step, mesh=mesh, in_specs=(act_spec, act_spec, in_spec, out_spec), out_specs=(in_spec, out_spec, P()), check_vma=False)
        return stepper(x_tokens, y_target, w_in, w_out)

    return sam_step
```

```python
import functools
import math

import jax
import jax.numpy as jnp
from jax import lax
from jax.experimental import pallas as pl
from jax.experimental.pallas import tpu as pltpu
from jax.sharding import PartitionSpec as P

MESH = pl.DeviceIdType.MESH
RHO_SCALE = 0.5
ETA = 1.0
HALF = 6
MB_IMAGES = 1
VMEM_LIMIT = 67043328
NN = (((1,), (0,)), ((), ()))
NT = (((1,), (1,)), ((), ()))
TN = (((0,), (0,)), ((), ()))
C0 = math.sqrt(2.0 / math.pi)
C1 = 0.044715
CHIPS = (1, 0, 2, 4, 6, 7)
STRIP = 128


def dot(lhs, rhs, dims):
    return lax.dot_general(lhs, rhs, dims, preferred_element_type=jnp.float32)


def chip_of(pos):
    return 2 * (pos - 1) + 3 * lax.div(5 - pos, 5) - lax.div(pos, 5)


def locate():
    m = lax.axis_index("model")
    d = lax.axis_index("data")
    x, core = lax.div(d, 2), lax.rem(d, 2)
    z, y = lax.div(m, 2), lax.rem(m, 2)
    pos = (1 - y) * (z + 1) + y * 5 * lax.div(z, 3)
    idle = y * (1 - lax.div(z, 3)) * jnp.minimum(z, 1)
    stage = (1 - x) * pos + x * (11 - pos)
    return m, x, core, stage, idle == 0


def stage_device(stage, core):
    plane = lax.div(stage, HALF)
    pos = (1 - plane) * stage + plane * (11 - stage)
    return chip_of(pos), plane * 2 + core


def step_kernel(cfg, win, wout, xin, yin,
                gin, gout, a_own, c_own, x_all, loss_out,
                a, c, ga, gc, rem, ybuf, hbuf, hout, zbuf, ubuf, ebuf, ebb,
                acc, nrm_send, nrm, loss_send,
                w_send, w_recv, w_loc, xy_send, xy_recv, xy_loc, stage_loc, t_send, t_recv, g_send, g_recv,
                hs, hr, es, er, stagger, n_send, n_recv, l_send, l_recv,
                s1, r1, s2, r2, s3, r3, s_loc):
    rows, sent, per_shard, n_mb, res_scale, rho, n_data = cfg
    m, x, core, stage, active = locate()
    depth, hidden = a.shape
    width = hidden // 8
    quarter = hidden // 4
    strips = quarter // STRIP
    shard_rows = per_shard * rows
    mine = x * 2 + core
    across = (1 - x) * 2 + core
    twin = x * 2 + (1 - core)
    prev_dev = stage_device(jnp.maximum(stage - 1, 0), core)
    next_dev = stage_device(jnp.minimum(stage + 1, 11), core)
    last = stage == 11

    def remote(src, dst, send, recv, dev):
        return pltpu.make_async_remote_copy(src, dst, send, recv, device_id=dev, device_id_type=MESH)

    barrier = pltpu.get_barrier_semaphore()
    here = m * 4 + mine
    for step in range(1, 32):
        there = lax.rem(here + step, 32)
        pl.semaphore_signal(barrier, inc=1, device_id=(lax.div(there, 4), lax.rem(there, 4)), device_id_type=MESH)
    pl.semaphore_wait(barrier, 31)

    def weight_ends(kind, layer, shard):
        sl = pl.ds(pl.multiple_of(shard * width, width), width)
        return (win.at[layer], a_own.at[:, sl]) if kind == 0 else (wout.at[layer], c_own.at[sl, :])

    def weight_copy(kind, j, shard):
        layer = x * HALF + j
        src, dst = weight_ends(kind, layer, shard)
        dest = chip_of((1 - x) * j + x * (5 - j))
        return dest, remote(src, dst, w_send.at[j], w_recv.at[shard], (dest, mine)), pltpu.make_async_copy(src, dst, w_loc)

    for kind in (0, 1):
        @pl.when(core == kind)
        def _(kind=kind):
            for j in range(HALF):
                dest, far, near = weight_copy(kind, j, m)

                @pl.when(m != dest)
                def _():
                    far.start()

                @pl.when(m == dest)
                def _():
                    near.start()

    own_rows = pl.ds(pl.multiple_of(x * shard_rows, shard_rows), shard_rows)
    xy_far = [remote(src, dst.at[own_rows, :], xy_send.at[i], xy_recv.at[i], (m, across)) for i, (src, dst) in enumerate(((xin, x_all), (yin, ybuf)))]
    xy_near = [pltpu.make_async_copy(src, dst.at[own_rows, :], xy_loc.at[i]) for i, (src, dst) in enumerate(((xin, x_all), (yin, ybuf)))]
    for copy in xy_far + xy_near:
        copy.start()
    for copy in xy_near + xy_far:
        copy.wait()

    def piece(kind, ref_a, ref_c, q):
        sl = pl.ds(pl.multiple_of(q * quarter, quarter), quarter)
        return ref_a.at[:, sl] if kind == 0 else ref_c.at[sl, :]

    def strip(kind, ref_a, ref_c, q, i):
        cols = pl.ds(pl.multiple_of(q * quarter, quarter), quarter)
        if kind == 0:
            return ref_a, (pl.ds(pl.multiple_of(i * STRIP, STRIP), STRIP), cols)
        return ref_c, (pl.ds(pl.multiple_of(q * quarter + i * STRIP, STRIP), STRIP), slice(None))

    def strip_rows(i):
        return pl.ds(pl.multiple_of(i * STRIP, STRIP), STRIP)

    def master_copy(kind, q):
        return pltpu.make_async_copy(piece(kind, a_own, c_own, q), rem.at[q], stage_loc.at[q])

    def twin_copy(kind, q):
        ref = piece(kind, a, c, q)
        return remote(ref, ref, t_send.at[q], t_recv.at[q], (m, twin))

    def grad_copy(kind, q):
        return remote(piece(kind, ga, gc, q), rem.at[q], g_send.at[q], g_recv.at[q], (m, twin))

    def load_weights(kind, scale):
        for q in range(4):
            if scale is None:
                for shard in (2 * q, 2 * q + 1):
                    far = remote(weight_ends(kind, 0, shard)[0], weight_ends(kind, 0, shard)[1], w_send.at[0], w_recv.at[shard], (m, mine))

                    @pl.when(m != shard)
                    def _():
                        far.wait_recv()

                    @pl.when(m == shard)
                    def _():
                        pltpu.make_async_copy(weight_ends(kind, 0, shard)[0], weight_ends(kind, 0, shard)[1], w_loc).wait()

                master_copy(kind, q).start()
            master_copy(kind, q).wait()

            def round_strip(i, carry):
                dst, where = strip(kind, a, c, q, i)
                value = rem[q, strip_rows(i), :]
                if scale is not None:
                    src, _ = strip(kind, ga, gc, q, i)
                    value = value + scale * src[where]
                dst[where] = value.astype(jnp.bfloat16)
                return carry

            lax.fori_loop(0, strips, round_strip, 0)
            twin_copy(kind, q).start()
        for q in range(4):
            twin_copy(kind, q).wait_send()
        for q in range(4):
            twin_copy(1 - kind, q).wait_recv()

    def block(mb):
        return pl.ds(pl.multiple_of(mb * rows, rows), rows)

    def h_copy(mb):
        return remote(hout.at[block(mb), :], hbuf.at[block(mb), :], hs.at[mb], hr.at[mb], next_dev)

    def e_copy(mb):
        ref = ebuf.at[pl.ds(pl.multiple_of(mb * rows, rows), sent), :]
        return remote(ref, ref, es.at[mb], er.at[mb], prev_dev)

    def forward(mb):
        h = hbuf[block(mb), :]
        mix = None
        for q in range(4):
            sl = slice(q * quarter, (q + 1) * quarter)
            z = dot(h, a[:, sl], NN).astype(jnp.bfloat16)
            zf = z.astype(jnp.float32)
            u = (zf * (0.5 * (1.0 + jnp.tanh(C0 * (zf + C1 * (zf * zf * zf)))))).astype(jnp.bfloat16)
            zbuf[block(mb), sl] = z
            ubuf[block(mb), sl] = u
            part = dot(u, c[sl, :], NN)
            mix = part if mix is None else mix + part
        return (h.astype(jnp.float32) + mix).astype(jnp.bfloat16)

    def backward(mb):
        e = ebuf[block(mb), :]
        eb = e.astype(jnp.bfloat16)
        ebb[block(mb), :] = eb
        back = None
        for q in range(4):
            sl = slice(q * quarter, (q + 1) * quarter)
            du = dot(eb, c[sl, :], NT)
            zf = zbuf[block(mb), sl].astype(jnp.float32)
            z2 = zf * zf
            t = jnp.tanh(C0 * (zf + C1 * (z2 * zf)))
            slope = 0.5 * (1.0 + t) + (0.5 * zf) * ((1.0 - t * t) * (C0 + (3.0 * C0 * C1) * z2))
            dz = (slope * du).astype(jnp.bfloat16)
            zbuf[block(mb), sl] = dz
            part = dot(dz, a[:, sl], NT)
            back = part if back is None else back + part
        ebuf[block(mb), :] = e + back

    def grad_piece(shard, q):
        span = pl.ds(shard * shard_rows, shard_rows)
        sl = pl.ds(pl.multiple_of(q * quarter, quarter), quarter)
        d_out = dot(ubuf[span, sl], ebb[span, :], TN).astype(jnp.bfloat16).astype(jnp.float32)
        gc[sl, :] = d_out if shard == 0 else gc[sl, :] + d_out
        d_in = dot(hbuf[span, :], zbuf[span, sl], TN).astype(jnp.bfloat16).astype(jnp.float32)
        ga[:, sl] = d_in if shard == 0 else ga[:, sl] + d_in

    def on_core(fn):
        for kind in (0, 1):
            @pl.when(core == kind)
            def _(kind=kind):
                fn(kind)

    def run_pass(p, carry):
        acc[...] = jnp.zeros_like(acc)

        @pl.when(stage == 0)
        def _():
            x_copy = pltpu.make_async_copy(x_all, hbuf, w_loc)
            x_copy.start()
            x_copy.wait()

            @pl.when(core == 1)
            def _():
                pl.semaphore_wait(stagger, 1)

        def forward_step(mb, carry):
            @pl.when(stage > 0)
            def _():
                h_copy(mb).wait_recv()

            new_h = forward(mb)

            @pl.when(stage < 11)
            def _():
                hout[block(mb), :] = new_h
                h_copy(mb).start()

            @pl.when(jnp.logical_and(stage == 0, jnp.logical_and(core == 0, mb == 0)))
            def _():
                pl.semaphore_signal(stagger, inc=1, device_id=(m, twin), device_id_type=MESH)

            @pl.when(last)
            def _():
                res = new_h.astype(jnp.float32) - ybuf[block(mb), :].astype(jnp.float32)
                acc[...] = acc[...] + jnp.sum(res * res, axis=0, keepdims=True)
                ebuf[block(mb), :] = res / res_scale
                backward(mb)
                e_copy(mb).start()

            return carry

        lax.fori_loop(0, n_mb, forward_step, 0)

        def fold(dst):
            total = acc[:, 0:128]
            for i in range(1, depth // 128):
                total = total + acc[:, i * 128:(i + 1) * 128]
            dst[...] = jnp.broadcast_to(total, dst.shape)

        @pl.when(jnp.logical_and(last, p == 1))
        def _():
            fold(loss_send)
            for step in range(32):
                row_copy = remote(loss_send, loss_out.at[core], l_send.at[step], l_recv.at[core], (step // 4, step % 4))

                @pl.when(here != step)
                def _():
                    row_copy.start()

            loss_out[core] = loss_send[...]
            for step in range(32):
                row_copy = remote(loss_send, loss_out.at[core], l_send.at[step], l_recv.at[core], (step // 4, step % 4))

                @pl.when(here != step)
                def _():
                    row_copy.wait_send()

        def backward_step(mb):
            @pl.when(stage < 11)
            def _():
                e_copy(mb).wait_recv()
                backward(mb)

                @pl.when(stage > 0)
                def _():
                    e_copy(mb).start()

        def first_shard(mb, carry):
            backward_step(mb)
            return carry

        def second_shard(q, carry):
            for k in range(per_shard // 4):
                backward_step(per_shard + q * (per_shard // 4) + k)
            grad_piece(0, q)
            return carry

        def tail_grads(q, carry):
            grad_piece(1, q)
            on_core(lambda kind: grad_copy(1 - kind, q).start())
            return carry

        lax.fori_loop(0, per_shard, first_shard, 0)
        lax.fori_loop(0, 4, second_shard, 0)
        lax.fori_loop(0, 4, tail_grads, 0)

        def drain(mb, carry):
            @pl.when(stage < 11)
            def _():
                h_copy(mb).wait_send()

            @pl.when(stage > 0)
            def _():
                e_copy(mb).wait_send()

            return carry

        lax.fori_loop(0, n_mb, drain, 0)

        def between(kind):
            acc[...] = jnp.zeros_like(acc)

            def total_quarter(q, carry):
                grad_copy(kind, q).wait_recv()

                def total_strip(i, carry):
                    ref, where = strip(kind, ga, gc, q, i)
                    total = (ref[where] + rem[q, strip_rows(i), :]) / n_data
                    ref[where] = total
                    acc[...] = acc[...] + jnp.sum(total * total, axis=0, keepdims=True)
                    return carry

                return lax.fori_loop(0, strips, total_strip, carry)

            lax.fori_loop(0, 4, total_quarter, 0)
            for q in range(4):
                master_copy(kind, q).start()
            fold(nrm_send)
            slot = stage * 2 + core

            def norm_copies():
                for s in range(12):
                    chip = CHIPS[s] if s < HALF else CHIPS[11 - s]
                    for k in range(2):
                        dev = (chip, (s // HALF) * 2 + k)
                        yield s * 2 + k, remote(nrm_send, nrm.at[slot], n_send.at[s * 2 + k], n_recv.at[slot], dev)

            for i, copy in norm_copies():
                @pl.when(slot != i)
                def _():
                    copy.start()

            nrm[slot] = nrm_send[...]
            for i, copy in norm_copies():
                @pl.when(slot != i)
                def _():
                    copy.wait_send()
                    remote(nrm_send, nrm.at[i], n_send.at[i], n_recv.at[i], (m, mine)).wait_recv()

            square = jnp.sum(jnp.sum(nrm[:, 0, :], axis=0, keepdims=True), axis=1, keepdims=True)
            for q in range(4):
                grad_copy(1 - kind, q).wait_send()
            load_weights(kind, rho / jnp.sqrt(square))

        @pl.when(p == 0)
        def _():
            on_core(between)

        return carry

    @pl.when(active)
    def _():
        ebuf[...] = jnp.zeros_like(ebuf)
        on_core(lambda kind: load_weights(kind, None))
        lax.fori_loop(0, 2, run_pass, 0)

    def scatter(kind):
        dst = gin if kind == 0 else gout
        other_dst = gout if kind == 0 else gin

        def ends(peer):
            sl = pl.ds(pl.multiple_of(peer * width, width), width)
            return ga.at[:, sl] if kind == 0 else gc.at[sl, :]

        def first_hop(peer, layer, slot):
            return remote(ends(peer), dst.at[layer], s1.at[peer], r1.at[slot], (peer, mine))

        def cross(layer, slot):
            return remote(dst.at[layer], dst.at[layer], s2.at[slot], r2.at[slot], (m, across))

        def to_twin(layer):
            return remote(dst.at[layer], dst.at[layer], s3.at[layer], r3.at[layer], (m, twin))

        def from_twin(layer):
            return remote(other_dst.at[layer], other_dst.at[layer], s3.at[layer], r3.at[layer], (m, twin))

        @pl.when(active)
        def _():
            def send_quarter(q, carry):
                grad_copy(kind, q).wait_recv()

                def total_strip(i, carry):
                    ref, where = strip(kind, ga, gc, q, i)
                    ref[where] = (ref[where] + rem[q, strip_rows(i), :]) / n_data
                    return carry

                lax.fori_loop(0, strips, total_strip, 0)
                for k in range(2):
                    peer = 2 * q + k

                    @pl.when(m != peer)
                    def _():
                        first_hop(peer, stage, stage - x * HALF).start()

                    @pl.when(m == peer)
                    def _():
                        pltpu.make_async_copy(ends(peer), dst.at[stage], s_loc).start()

                return carry

            lax.fori_loop(0, 4, send_quarter, 0)

        for slot in reversed(range(HALF)):
            layer = x * HALF + slot
            is_mine = jnp.logical_and(active, stage == layer)

            @pl.when(is_mine)
            def _():
                pltpu.make_async_copy(ends(0), dst.at[layer], s_loc).wait()

            @pl.when(jnp.logical_not(is_mine))
            def _():
                first_hop(0, layer, slot).wait_recv()

            cross(layer, slot).start()
            to_twin(layer).start()
        for slot in reversed(range(HALF)):
            layer = (1 - x) * HALF + slot
            cross(layer, slot).wait_recv()
            to_twin(layer).start()
        for layer in range(2 * HALF):
            from_twin(layer).wait_recv()

        @pl.when(active)
        def _():
            for peer in range(8):
                @pl.when(m != peer)
                def _():
                    first_hop(peer, stage, stage - x * HALF).wait_send()

            for q in range(4):
                grad_copy(1 - kind, q).wait_send()

        for slot in range(HALF):
            cross(x * HALF + slot, slot).wait_send()
        for layer in range(2 * HALF):
            to_twin(layer).wait_send()

        for j in range(HALF):
            dest, far, _ = weight_copy(kind, j, m)

            @pl.when(m != dest)
            def _():
                far.wait_send()

    on_core(scatter)

    for k in range(2):
        @pl.when(jnp.logical_not(jnp.logical_and(active, jnp.logical_and(last, core == k))))
        def _():
            remote(loss_send, loss_out.at[k], l_send.at[0], l_recv.at[k], (m, mine)).wait_recv()


def run_step(win, wout, xin, yin, rows, sent, per_shard, res_scale, rho, n_data):
    layers, depth, width = win.shape
    hidden = width * 8
    total = 2 * per_shard * rows
    n_mb = 2 * per_shard
    shape = jax.ShapeDtypeStruct
    dma = pltpu.SemaphoreType.DMA
    f32, bf16 = jnp.float32, jnp.bfloat16
    any_space = pl.BlockSpec(memory_space=pl.ANY)
    return pl.pallas_call(
        functools.partial(step_kernel, (rows, sent, per_shard, n_mb, res_scale, rho, n_data)),
        out_shape=[shape(win.shape, f32), shape(wout.shape, f32), shape((depth, hidden), f32), shape((hidden, depth), f32), shape((total, depth), bf16), shape((2, 8, 128), f32)],
        in_specs=[any_space] * 4,
        out_specs=[any_space] * 5 + [pl.BlockSpec(memory_space=pltpu.VMEM)],
        scratch_shapes=[
            pltpu.VMEM((depth, hidden), bf16),
            pltpu.VMEM((hidden, depth), bf16),
            pltpu.VMEM((depth, hidden), f32),
            pltpu.VMEM((hidden, depth), f32),
            pltpu.VMEM((4, depth, depth), f32),
            pltpu.VMEM((total, depth), bf16),
            pltpu.VMEM((total, depth), bf16),
            pltpu.VMEM((total, depth), bf16),
            pltpu.VMEM((total, hidden), bf16),
            pltpu.VMEM((total, hidden), bf16),
            pltpu.VMEM((total, depth), f32),
            pltpu.VMEM((total, depth), bf16),
            pltpu.VMEM((1, depth), f32),
            pltpu.VMEM((8, 128), f32),
            pltpu.VMEM((24, 8, 128), f32),
            pltpu.VMEM((8, 128), f32),
            dma((HALF,)), dma((8,)), dma, dma((2,)), dma((2,)), dma((2,)), dma((4,)), dma((4,)), dma((4,)), dma((4,)), dma((4,)),
            dma((n_mb,)), dma((n_mb,)), dma((n_mb,)), dma((n_mb,)), pltpu.SemaphoreType.REGULAR,
            dma((24,)), dma((24,)), dma((32,)), dma((2,)),
            dma((8,)), dma((HALF,)), dma((HALF,)), dma((HALF,)), dma((2 * HALF,)), dma((2 * HALF,)), dma,
        ],
        compiler_params=pltpu.CompilerParams(collective_id=0, has_side_effects=True, vmem_limit_bytes=VMEM_LIMIT),
        name="sam_step",
    )(win, wout, xin, yin)


def solution(mesh):
    act_spec = P("data", None, None)
    in_spec = P(None, None, "model")
    out_spec = P(None, "model", None)

    def sam_step(x_tokens, y_target, w_in, w_out):
        rho = RHO_SCALE * math.sqrt(x_tokens.shape[-1] / w_in.shape[-1])
        elem_total = x_tokens.size
        n_data = mesh.shape["data"]

        def local_step(x_blk, y_blk, win_loc, wout_loc):
            images, seq, depth = x_blk.shape
            raw = MB_IMAGES * seq
            rows = (raw + 15) // 16 * 16
            sent = (raw + 7) // 8 * 8
            per_shard = images // MB_IMAGES

            def flat(blk):
                mbs = blk.reshape(per_shard, raw, depth)
                return jnp.pad(mbs, ((0, 0), (0, rows - raw), (0, 0))).reshape(per_shard * rows, depth)

            res_scale = float(images * seq * depth)
            grad_in, grad_out, _, _, _, loss = run_step(win_loc, wout_loc, flat(x_blk), flat(y_blk), rows, sent, per_shard, res_scale, rho, n_data)
            loss_val = 0.5 * jnp.sum(loss[:, 0, :]) / elem_total
            return win_loc - ETA * grad_in, wout_loc - ETA * grad_out, loss_val

        stepper = jax.shard_map(local_step, mesh=mesh, in_specs=(act_spec, act_spec, in_spec, out_spec), out_specs=(in_spec, out_spec, P()), check_vma=False)
        return stepper(x_tokens, y_target, w_in, w_out)

    return sam_step
```

```python
import functools
import math

import jax
import jax.numpy as jnp
from jax import lax
from jax.experimental import pallas as pl
from jax.experimental.pallas import tpu as pltpu
from jax.sharding import PartitionSpec as P

MESH = pl.DeviceIdType.MESH
RHO_SCALE = 0.5
ETA = 1.0
HALF = 6
MB_IMAGES = 1
VMEM_LIMIT = 67043328
NN = (((1,), (0,)), ((), ()))
NT = (((1,), (1,)), ((), ()))
TN = (((0,), (0,)), ((), ()))
C0 = math.sqrt(2.0 / math.pi)
C1 = 0.044715
CHIPS = (1, 0, 2, 4, 6, 7)
STRIP = 128


def dot(lhs, rhs, dims):
    return lax.dot_general(lhs, rhs, dims, preferred_element_type=jnp.float32)


def chip_of(pos):
    return 2 * (pos - 1) + 3 * lax.div(5 - pos, 5) - lax.div(pos, 5)


def locate():
    m = lax.axis_index("model")
    d = lax.axis_index("data")
    x, core = lax.div(d, 2), lax.rem(d, 2)
    z, y = lax.div(m, 2), lax.rem(m, 2)
    pos = (1 - y) * (z + 1) + y * 5 * lax.div(z, 3)
    idle = y * (1 - lax.div(z, 3)) * jnp.minimum(z, 1)
    stage = (1 - x) * pos + x * (11 - pos)
    return m, x, core, stage, idle == 0


def stage_device(stage, core):
    plane = lax.div(stage, HALF)
    pos = (1 - plane) * stage + plane * (11 - stage)
    return chip_of(pos), plane * 2 + core


def step_kernel(cfg, win, wout, xin, yin,
                gin, gout, a_own, c_own, x_all, loss_out,
                a, c, ga, gc, rem, ybuf, hbuf, hout, zbuf, ubuf, ebuf, ebb,
                acc, nrm_send, nrm, loss_send,
                w_send, w_recv, w_loc, xy_send, xy_recv, xy_loc, stage_loc, t_send, t_recv, g_send, g_recv,
                hs, hr, es, er, stagger, n_send, n_recv, l_send, l_recv,
                s1, r1, s2, r2, s3, r3, s_loc):
    rows, sent, per_shard, n_mb, res_scale, rho, n_data = cfg
    m, x, core, stage, active = locate()
    depth, hidden = a.shape
    width = hidden // 8
    quarter = hidden // 4
    strips = quarter // STRIP
    shard_rows = per_shard * rows
    mine = x * 2 + core
    across = (1 - x) * 2 + core
    twin = x * 2 + (1 - core)
    prev_dev = stage_device(jnp.maximum(stage - 1, 0), core)
    next_dev = stage_device(jnp.minimum(stage + 1, 11), core)
    last = stage == 11
    right = lax.div(m, 4)

    def near_first(i):
        return right * (3 - i) + (1 - right) * i

    def remote(src, dst, send, recv, dev):
        return pltpu.make_async_remote_copy(src, dst, send, recv, device_id=dev, device_id_type=MESH)

    barrier = pltpu.get_barrier_semaphore()
    here = m * 4 + mine
    for step in range(1, 32):
        there = lax.rem(here + step, 32)
        pl.semaphore_signal(barrier, inc=1, device_id=(lax.div(there, 4), lax.rem(there, 4)), device_id_type=MESH)
    pl.semaphore_wait(barrier, 31)

    def weight_ends(kind, layer, shard):
        sl = pl.ds(pl.multiple_of(shard * width, width), width)
        return (win.at[layer], a_own.at[:, sl]) if kind == 0 else (wout.at[layer], c_own.at[sl, :])

    def weight_copy(kind, j, shard):
        layer = x * HALF + j
        src, dst = weight_ends(kind, layer, shard)
        dest = chip_of((1 - x) * j + x * (5 - j))
        return dest, remote(src, dst, w_send.at[j], w_recv.at[shard], (dest, mine)), pltpu.make_async_copy(src, dst, w_loc)

    for kind in (0, 1):
        @pl.when(core == kind)
        def _(kind=kind):
            for j in range(HALF):
                dest, far, near = weight_copy(kind, j, m)

                @pl.when(m != dest)
                def _():
                    far.start()

                @pl.when(m == dest)
                def _():
                    near.start()

    own_rows = pl.ds(pl.multiple_of(x * shard_rows, shard_rows), shard_rows)
    xy_far = [remote(src, dst.at[own_rows, :], xy_send.at[i], xy_recv.at[i], (m, across)) for i, (src, dst) in enumerate(((xin, x_all), (yin, ybuf)))]
    xy_near = [pltpu.make_async_copy(src, dst.at[own_rows, :], xy_loc.at[i]) for i, (src, dst) in enumerate(((xin, x_all), (yin, ybuf)))]
    for copy in xy_far + xy_near:
        copy.start()
    for copy in xy_near + xy_far:
        copy.wait()

    def piece(kind, ref_a, ref_c, q):
        sl = pl.ds(pl.multiple_of(q * quarter, quarter), quarter)
        return ref_a.at[:, sl] if kind == 0 else ref_c.at[sl, :]

    def strip(kind, ref_a, ref_c, q, i):
        cols = pl.ds(pl.multiple_of(q * quarter, quarter), quarter)
        if kind == 0:
            return ref_a, (pl.ds(pl.multiple_of(i * STRIP, STRIP), STRIP), cols)
        return ref_c, (pl.ds(pl.multiple_of(q * quarter + i * STRIP, STRIP), STRIP), slice(None))

    def strip_rows(i):
        return pl.ds(pl.multiple_of(i * STRIP, STRIP), STRIP)

    def master_copy(kind, q):
        return pltpu.make_async_copy(piece(kind, a_own, c_own, q), rem.at[q], stage_loc.at[q])

    def twin_copy(kind, q):
        ref = piece(kind, a, c, q)
        return remote(ref, ref, t_send.at[q], t_recv.at[q], (m, twin))

    def grad_copy(kind, q):
        return remote(piece(kind, ga, gc, q), rem.at[q], g_send.at[q], g_recv.at[q], (m, twin))

    def load_weights(kind, scale):
        for q in range(4):
            if scale is None:
                for shard in (2 * q, 2 * q + 1):
                    far = remote(weight_ends(kind, 0, shard)[0], weight_ends(kind, 0, shard)[1], w_send.at[0], w_recv.at[shard], (m, mine))

                    @pl.when(m != shard)
                    def _():
                        far.wait_recv()

                    @pl.when(m == shard)
                    def _():
                        pltpu.make_async_copy(weight_ends(kind, 0, shard)[0], weight_ends(kind, 0, shard)[1], w_loc).wait()

                master_copy(kind, q).start()
            master_copy(kind, q).wait()

            def round_strip(i, carry):
                dst, where = strip(kind, a, c, q, i)
                value = rem[q, strip_rows(i), :]
                if scale is not None:
                    src, _ = strip(kind, ga, gc, q, i)
                    value = value + scale * src[where]
                dst[where] = value.astype(jnp.bfloat16)
                return carry

            lax.fori_loop(0, strips, round_strip, 0)
            twin_copy(kind, q).start()
        for q in range(4):
            twin_copy(kind, q).wait_send()
        for q in range(4):
            twin_copy(1 - kind, q).wait_recv()

    def block(mb):
        return pl.ds(pl.multiple_of(mb * rows, rows), rows)

    def h_copy(mb):
        return remote(hout.at[block(mb), :], hbuf.at[block(mb), :], hs.at[mb], hr.at[mb], next_dev)

    def e_copy(mb):
        ref = ebuf.at[pl.ds(pl.multiple_of(mb * rows, rows), sent), :]
        return remote(ref, ref, es.at[mb], er.at[mb], prev_dev)

    def forward(mb):
        h = hbuf[block(mb), :]
        mix = None
        for q in range(4):
            sl = slice(q * quarter, (q + 1) * quarter)
            z = dot(h, a[:, sl], NN).astype(jnp.bfloat16)
            zf = z.astype(jnp.float32)
            u = (zf * (0.5 * (1.0 + jnp.tanh(C0 * (zf + C1 * (zf * zf * zf)))))).astype(jnp.bfloat16)
            zbuf[block(mb), sl] = z
            ubuf[block(mb), sl] = u
            part = dot(u, c[sl, :], NN)
            mix = part if mix is None else mix + part
        return (h.astype(jnp.float32) + mix).astype(jnp.bfloat16)

    def backward(mb):
        e = ebuf[block(mb), :]
        eb = e.astype(jnp.bfloat16)
        ebb[block(mb), :] = eb
        back = None
        for q in range(4):
            sl = slice(q * quarter, (q + 1) * quarter)
            du = dot(eb, c[sl, :], NT)
            zf = zbuf[block(mb), sl].astype(jnp.float32)
            z2 = zf * zf
            t = jnp.tanh(C0 * (zf + C1 * (z2 * zf)))
            slope = 0.5 * (1.0 + t) + (0.5 * zf) * ((1.0 - t * t) * (C0 + (3.0 * C0 * C1) * z2))
            dz = (slope * du).astype(jnp.bfloat16)
            zbuf[block(mb), sl] = dz
            part = dot(dz, a[:, sl], NT)
            back = part if back is None else back + part
        ebuf[block(mb), :] = e + back

    def grad_piece(shard, q):
        span = pl.ds(shard * shard_rows, shard_rows)
        sl = pl.ds(pl.multiple_of(q * quarter, quarter), quarter)
        d_out = dot(ubuf[span, sl], ebb[span, :], TN).astype(jnp.bfloat16).astype(jnp.float32)
        gc[sl, :] = d_out if shard == 0 else gc[sl, :] + d_out
        d_in = dot(hbuf[span, :], zbuf[span, sl], TN).astype(jnp.bfloat16).astype(jnp.float32)
        ga[:, sl] = d_in if shard == 0 else ga[:, sl] + d_in

    def on_core(fn):
        for kind in (0, 1):
            @pl.when(core == kind)
            def _(kind=kind):
                fn(kind)

    def run_pass(p, carry):
        acc[...] = jnp.zeros_like(acc)

        @pl.when(stage == 0)
        def _():
            x_copy = pltpu.make_async_copy(x_all, hbuf, w_loc)
            x_copy.start()
            x_copy.wait()

            @pl.when(core == 1)
            def _():
                pl.semaphore_wait(stagger, 1)

        def forward_step(mb, carry):
            @pl.when(stage > 0)
            def _():
                h_copy(mb).wait_recv()

            new_h = forward(mb)

            @pl.when(stage < 11)
            def _():
                hout[block(mb), :] = new_h
                h_copy(mb).start()

            @pl.when(jnp.logical_and(stage == 0, jnp.logical_and(core == 0, mb == 0)))
            def _():
                pl.semaphore_signal(stagger, inc=1, device_id=(m, twin), device_id_type=MESH)

            @pl.when(last)
            def _():
                res = new_h.astype(jnp.float32) - ybuf[block(mb), :].astype(jnp.float32)
                acc[...] = acc[...] + jnp.sum(res * res, axis=0, keepdims=True)
                ebuf[block(mb), :] = res / res_scale
                backward(mb)
                e_copy(mb).start()

            return carry

        lax.fori_loop(0, n_mb, forward_step, 0)

        def fold(dst):
            total = acc[:, 0:128]
            for i in range(1, depth // 128):
                total = total + acc[:, i * 128:(i + 1) * 128]
            dst[...] = jnp.broadcast_to(total, dst.shape)

        @pl.when(jnp.logical_and(last, p == 1))
        def _():
            fold(loss_send)
            for step in range(32):
                row_copy = remote(loss_send, loss_out.at[core], l_send.at[step], l_recv.at[core], (step // 4, step % 4))

                @pl.when(here != step)
                def _():
                    row_copy.start()

            loss_out[core] = loss_send[...]
            for step in range(32):
                row_copy = remote(loss_send, loss_out.at[core], l_send.at[step], l_recv.at[core], (step // 4, step % 4))

                @pl.when(here != step)
                def _():
                    row_copy.wait_send()

        def backward_step(mb):
            @pl.when(stage < 11)
            def _():
                e_copy(mb).wait_recv()
                backward(mb)

                @pl.when(stage > 0)
                def _():
                    e_copy(mb).start()

        def first_shard(mb, carry):
            backward_step(mb)
            return carry

        def second_shard(q, carry):
            for k in range(per_shard // 4):
                backward_step(per_shard + q * (per_shard // 4) + k)
            grad_piece(0, q)
            return carry

        def tail_grads(i, carry):
            q = near_first(i)
            grad_piece(1, q)
            on_core(lambda kind: grad_copy(1 - kind, q).start())
            return carry

        lax.fori_loop(0, per_shard, first_shard, 0)
        lax.fori_loop(0, 4, second_shard, 0)
        lax.fori_loop(0, 4, tail_grads, 0)

        def drain(mb, carry):
            @pl.when(stage < 11)
            def _():
                h_copy(mb).wait_send()

            @pl.when(stage > 0)
            def _():
                e_copy(mb).wait_send()

            return carry

        lax.fori_loop(0, n_mb, drain, 0)

        def between(kind):
            acc[...] = jnp.zeros_like(acc)

            def total_quarter(q, carry):
                grad_copy(kind, q).wait_recv()

                def total_strip(i, carry):
                    ref, where = strip(kind, ga, gc, q, i)
                    total = (ref[where] + rem[q, strip_rows(i), :]) / n_data
                    ref[where] = total
                    acc[...] = acc[...] + jnp.sum(total * total, axis=0, keepdims=True)
                    return carry

                return lax.fori_loop(0, strips, total_strip, carry)

            lax.fori_loop(0, 4, total_quarter, 0)
            for q in range(4):
                master_copy(kind, q).start()
            fold(nrm_send)
            slot = stage * 2 + core

            def norm_copies():
                for s in range(12):
                    chip = CHIPS[s] if s < HALF else CHIPS[11 - s]
                    for k in range(2):
                        dev = (chip, (s // HALF) * 2 + k)
                        yield s * 2 + k, remote(nrm_send, nrm.at[slot], n_send.at[s * 2 + k], n_recv.at[slot], dev)

            for i, copy in norm_copies():
                @pl.when(slot != i)
                def _():
                    copy.start()

            nrm[slot] = nrm_send[...]
            for i, copy in norm_copies():
                @pl.when(slot != i)
                def _():
                    copy.wait_send()
                    remote(nrm_send, nrm.at[i], n_send.at[i], n_recv.at[i], (m, mine)).wait_recv()

            square = jnp.sum(jnp.sum(nrm[:, 0, :], axis=0, keepdims=True), axis=1, keepdims=True)
            for q in range(4):
                grad_copy(1 - kind, q).wait_send()
            load_weights(kind, rho / jnp.sqrt(square))

        @pl.when(p == 0)
        def _():
            on_core(between)

        return carry

    @pl.when(active)
    def _():
        ebuf[...] = jnp.zeros_like(ebuf)
        on_core(lambda kind: load_weights(kind, None))
        lax.fori_loop(0, 2, run_pass, 0)

    def scatter(kind):
        dst = gin if kind == 0 else gout
        other_dst = gout if kind == 0 else gin

        def ends(peer):
            sl = pl.ds(pl.multiple_of(peer * width, width), width)
            return ga.at[:, sl] if kind == 0 else gc.at[sl, :]

        def first_hop(peer, layer, slot):
            return remote(ends(peer), dst.at[layer], s1.at[peer], r1.at[slot], (peer, mine))

        def cross(layer, slot):
            return remote(dst.at[layer], dst.at[layer], s2.at[slot], r2.at[slot], (m, across))

        def to_twin(layer):
            return remote(dst.at[layer], dst.at[layer], s3.at[layer], r3.at[layer], (m, twin))

        def from_twin(layer):
            return remote(other_dst.at[layer], other_dst.at[layer], s3.at[layer], r3.at[layer], (m, twin))

        @pl.when(active)
        def _():
            def send_quarter(i, carry):
                q = near_first(i)
                grad_copy(kind, q).wait_recv()

                def total_strip(j, carry):
                    ref, where = strip(kind, ga, gc, q, j)
                    ref[where] = (ref[where] + rem[q, strip_rows(j), :]) / n_data
                    return carry

                lax.fori_loop(0, strips, total_strip, 0)
                for k in range(2):
                    peer = 2 * q + k

                    @pl.when(m != peer)
                    def _():
                        first_hop(peer, stage, stage - x * HALF).start()

                    @pl.when(m == peer)
                    def _():
                        pltpu.make_async_copy(ends(peer), dst.at[stage], s_loc).start()

                return carry

            lax.fori_loop(0, 4, send_quarter, 0)

        for slot in reversed(range(HALF)):
            layer = x * HALF + slot
            is_mine = jnp.logical_and(active, stage == layer)

            @pl.when(is_mine)
            def _():
                pltpu.make_async_copy(ends(0), dst.at[layer], s_loc).wait()

            @pl.when(jnp.logical_not(is_mine))
            def _():
                first_hop(0, layer, slot).wait_recv()

            cross(layer, slot).start()
            to_twin(layer).start()
        for slot in reversed(range(HALF)):
            layer = (1 - x) * HALF + slot
            cross(layer, slot).wait_recv()
            to_twin(layer).start()
        for layer in range(2 * HALF):
            from_twin(layer).wait_recv()

        @pl.when(active)
        def _():
            for peer in range(8):
                @pl.when(m != peer)
                def _():
                    first_hop(peer, stage, stage - x * HALF).wait_send()

            for q in range(4):
                grad_copy(1 - kind, q).wait_send()

        for slot in range(HALF):
            cross(x * HALF + slot, slot).wait_send()
        for layer in range(2 * HALF):
            to_twin(layer).wait_send()

        for j in range(HALF):
            dest, far, _ = weight_copy(kind, j, m)

            @pl.when(m != dest)
            def _():
                far.wait_send()

    on_core(scatter)

    for k in range(2):
        @pl.when(jnp.logical_not(jnp.logical_and(active, jnp.logical_and(last, core == k))))
        def _():
            remote(loss_send, loss_out.at[k], l_send.at[0], l_recv.at[k], (m, mine)).wait_recv()


def run_step(win, wout, xin, yin, rows, sent, per_shard, res_scale, rho, n_data):
    layers, depth, width = win.shape
    hidden = width * 8
    total = 2 * per_shard * rows
    n_mb = 2 * per_shard
    shape = jax.ShapeDtypeStruct
    dma = pltpu.SemaphoreType.DMA
    f32, bf16 = jnp.float32, jnp.bfloat16
    any_space = pl.BlockSpec(memory_space=pl.ANY)
    return pl.pallas_call(
        functools.partial(step_kernel, (rows, sent, per_shard, n_mb, res_scale, rho, n_data)),
        out_shape=[shape(win.shape, f32), shape(wout.shape, f32), shape((depth, hidden), f32), shape((hidden, depth), f32), shape((total, depth), bf16), shape((2, 8, 128), f32)],
        in_specs=[any_space] * 4,
        out_specs=[any_space] * 5 + [pl.BlockSpec(memory_space=pltpu.VMEM)],
        scratch_shapes=[
            pltpu.VMEM((depth, hidden), bf16),
            pltpu.VMEM((hidden, depth), bf16),
            pltpu.VMEM((depth, hidden), f32),
            pltpu.VMEM((hidden, depth), f32),
            pltpu.VMEM((4, depth, depth), f32),
            pltpu.VMEM((total, depth), bf16),
            pltpu.VMEM((total, depth), bf16),
            pltpu.VMEM((total, depth), bf16),
            pltpu.VMEM((total, hidden), bf16),
            pltpu.VMEM((total, hidden), bf16),
            pltpu.VMEM((total, depth), f32),
            pltpu.VMEM((total, depth), bf16),
            pltpu.VMEM((1, depth), f32),
            pltpu.VMEM((8, 128), f32),
            pltpu.VMEM((24, 8, 128), f32),
            pltpu.VMEM((8, 128), f32),
            dma((HALF,)), dma((8,)), dma, dma((2,)), dma((2,)), dma((2,)), dma((4,)), dma((4,)), dma((4,)), dma((4,)), dma((4,)),
            dma((n_mb,)), dma((n_mb,)), dma((n_mb,)), dma((n_mb,)), pltpu.SemaphoreType.REGULAR,
            dma((24,)), dma((24,)), dma((32,)), dma((2,)),
            dma((8,)), dma((HALF,)), dma((HALF,)), dma((HALF,)), dma((2 * HALF,)), dma((2 * HALF,)), dma,
        ],
        compiler_params=pltpu.CompilerParams(collective_id=0, has_side_effects=True, vmem_limit_bytes=VMEM_LIMIT),
        name="sam_step",
    )(win, wout, xin, yin)


def solution(mesh):
    act_spec = P("data", None, None)
    in_spec = P(None, None, "model")
    out_spec = P(None, "model", None)

    def sam_step(x_tokens, y_target, w_in, w_out):
        rho = RHO_SCALE * math.sqrt(x_tokens.shape[-1] / w_in.shape[-1])
        elem_total = x_tokens.size
        n_data = mesh.shape["data"]

        def local_step(x_blk, y_blk, win_loc, wout_loc):
            images, seq, depth = x_blk.shape
            raw = MB_IMAGES * seq
            rows = (raw + 15) // 16 * 16
            sent = (raw + 7) // 8 * 8
            per_shard = images // MB_IMAGES

            def flat(blk):
                mbs = blk.reshape(per_shard, raw, depth)
                return jnp.pad(mbs, ((0, 0), (0, rows - raw), (0, 0))).reshape(per_shard * rows, depth)

            res_scale = float(images * seq * depth)
            grad_in, grad_out, _, _, _, loss = run_step(win_loc, wout_loc, flat(x_blk), flat(y_blk), rows, sent, per_shard, res_scale, rho, n_data)
            loss_val = 0.5 * jnp.sum(loss[:, 0, :]) / elem_total
            return win_loc - ETA * grad_in, wout_loc - ETA * grad_out, loss_val

        stepper = jax.shard_map(local_step, mesh=mesh, in_specs=(act_spec, act_spec, in_spec, out_spec), out_specs=(in_spec, out_spec, P()), check_vma=False)
        return stepper(x_tokens, y_target, w_in, w_out)

    return sam_step
```
